8 devices in a mesh: batch: 1 (over z), gz: 2 (over y), gy: 2 (over x), gx: 2 (over core).
Axes of the slice: x: 2, y: 2, z: 1, core: 2. Of those that a mesh axis runs over, the one named last changes fastest.
Arguments:
- u_init: float32 [64, 128, 128], P(('batch', 'gx'), 'gy', 'gz')
- f_rhs: float32 [64, 128, 128], P(('batch', 'gx'), 'gy', 'gz')
- kappa_cell: float32 [64, 128, 128], P(('batch', 'gx'), 'gy', 'gz')
- stencil_w: float32 [26], replicated
- omega_sweep: float32 [32], replicated
Outputs:
- output: float32 [64, 128, 128], P(('batch', 'gx'), 'gy', 'gz')
All inputs are finite; a program needn't handle non-finite values.
Results may differ from the reference program's by a relative error of at most 0.001.
Values are sent between devices in bfloat16 or wider.
A program may use at most 1 GiB of HBM per device.

```python
import math
import jax
import jax.numpy as jnp
from jax import lax

GRID_X = 64
GRID_Y = 128
GRID_Z = 128
SWEEPS = 32


def offset_list():
    unit_steps = (-1, 0, 1)
    return [(a, b, c) for a in unit_steps for b in unit_steps for c in unit_steps if (a, b, c) != (0, 0, 0)]


def shifted(array_in, offset):
    return jnp.roll(array_in, (-offset[0], -offset[1], -offset[2]), axis=(0, 1, 2))


def setup_inputs(seed: int = 0, part: int = 0) -> dict:
    root_key = jax.random.key(seed)
    shared_key, part_root = jax.random.split(root_key)
    part_key = jax.random.fold_in(part_root, part)
    key_u, key_f, key_kappa = jax.random.split(part_key, 3)
    key_w, key_omega = jax.random.split(shared_key)
    grid_shape = (GRID_X, GRID_Y, GRID_Z)
    u_init = jax.random.normal(key_u, grid_shape, jnp.float32)
    f_rhs = 30.0 * jax.random.normal(key_f, grid_shape, jnp.float32)
    kappa_cell = jnp.exp(jax.random.uniform(key_kappa, grid_shape, jnp.float32, 0.0, math.log(10.0)))
    stencil_w = jax.random.uniform(key_w, (26,), jnp.float32, 0.5, 1.5)
    omega_sweep = jax.random.uniform(key_omega, (SWEEPS,), jnp.float32, 0.6, 1.0)
    return dict(u_init=u_init, f_rhs=f_rhs, kappa_cell=kappa_cell, stencil_w=stencil_w, omega_sweep=omega_sweep)


def reference(u_init, f_rhs, kappa_cell, stencil_w, omega_sweep):
    offsets = offset_list()
    diag_total = jnp.zeros_like(kappa_cell)
    for w_idx, offset in enumerate(offsets):
        diag_total = diag_total + stencil_w[w_idx] * (0.5 * (kappa_cell + shifted(kappa_cell, offset)))

    def sweep_once(u_cur, relax_now):
        applied = jnp.zeros_like(u_cur)
        for w_idx, offset in enumerate(offsets):
            coef_io = stencil_w[w_idx] * (0.5 * (kappa_cell + shifted(kappa_cell, offset)))
            applied = applied + coef_io * (u_cur - shifted(u_cur, offset))
        return u_cur + relax_now * (f_rhs - applied) / diag_total, None

    u_final, unused = lax.scan(sweep_once, u_init, omega_sweep)
    return u_final
```

```python
import functools

import jax
import jax.numpy as jnp
from jax import lax
from jax.experimental import pallas as pl
from jax.experimental.pallas import tpu as pltpu
from jax.sharding import PartitionSpec as P

MESH = pl.DeviceIdType.MESH
S = 4
ZB = 2
NZ, NU, LANES = 32, 32, 128
PAD = 16
ROWS = 56
ZE = NZ + 2 * S
FOLD = PAD + NU
SCALE = 2.0 ** -9
NCOPY = 2 + 3 * S
OFFSETS = [(a, b, c) for a in (-1, 0, 1) for b in (-1, 0, 1) for c in (-1, 0, 1) if (a, b, c) != (0, 0, 0)]
INDEX = {o: m for m, o in enumerate(OFFSETS)}


def swap_pairs(v, even):
    return jnp.where(even, pltpu.roll(v, LANES - 1, 1), pltpu.roll(v, 1, 1))


def exchange_copies(buf, send_sem, recv_sem, peers):
    low, high, gy, gylow, gyhigh = peers
    body = pl.ds(PAD, NU + 1)
    own = pl.ds(S, NZ)
    first, last = pl.ds(S, S), pl.ds(NZ, S)
    below, above = pl.ds(0, S), pl.ds(S + NZ, S)
    plan = [(first, body, above, body, low), (last, body, below, body, high)]
    for j in range(S):
        src, dst = pl.ds(PAD + j, 1), pl.ds(PAD - 1 - j, 1)
        plan.append((own, src, own, dst, gy))
        plan.append((first, src, above, dst, gylow))
        plan.append((last, src, below, dst, gyhigh))
    return [
        pltpu.make_async_remote_copy(
            src_ref=buf.at[sz, su, :],
            dst_ref=buf.at[dz, du, :],
            send_sem=send_sem.at[n],
            recv_sem=recv_sem.at[n],
            device_id=peer,
            device_id_type=MESH,
        )
        for n, (sz, su, dz, du, peer) in enumerate(plan)
    ]


def rows_loop(n_rows, block):
    full = n_rows // ZB

    def body(i, carry):
        block(i * ZB, ZB)
        return carry

    lax.fori_loop(0, full, body, 0)
    if n_rows % ZB:
        block(full * ZB, n_rows % ZB)


def load_window(ref, z0, count, base):
    return [
        [ref[z0 + dz, pl.ds(base + du, 8), :] for du in (-1, 0, 1)]
        for dz in range(-1, count + 1)
    ]


def kernel(n_sweeps, w_ref, om_ref, u_ref, f_ref, k_ref, o_ref,
           abuf, bbuf, cbuf, kbuf, fbuf, idbuf, tbuf,
           in_sem, send_sem, recv_sem, ksend, krecv, fsend, frecv):
    gz, gy, gx = lax.axis_index("gz"), lax.axis_index("gy"), lax.axis_index("gx")
    other = 1 - gx

    def dev(z, y, x):
        return {"batch": lax.axis_index("batch"), "gz": z, "gy": y, "gx": x}

    z_low, z_high = (gz + 1 - gx) % 2, (gz + gx) % 2
    peers = (dev(z_low, gy, other), dev(z_high, gy, other), dev(gz, 1 - gy, gx),
             dev(z_low, 1 - gy, other), dev(z_high, 1 - gy, other))
    own = (pl.ds(S, NZ), pl.ds(PAD, NU))

    loads = [
        pltpu.make_async_copy(src, dst.at[own[0], own[1], :], in_sem.at[n])
        for n, (src, dst) in enumerate(((k_ref, kbuf), (u_ref, abuf.at[0]), (f_ref, fbuf)))
    ]
    for copy in loads:
        copy.start()
    barrier = pltpu.get_barrier_semaphore()
    for peer in peers:
        pl.semaphore_signal(barrier, inc=1, device_id=peer, device_id_type=MESH)
    pl.semaphore_wait(barrier, len(peers))

    lane = lax.broadcasted_iota(jnp.int32, (8, LANES), 1)
    even = lane % 2 == 0
    upright = lane % 2 == gy

    for copy in loads:
        copy.wait()

    def fold(ref, z0, count):
        def body(i, carry):
            v = swap_pairs(ref[z0 + i, pl.ds(FOLD - 8, 8), :], even)
            ref[z0 + i, pl.ds(FOLD, 1), :] = v[7:8, :]
            return carry
        lax.fori_loop(0, count, body, 0)

    fold(kbuf, S, NZ)
    fold(abuf.at[0], S, NZ)
    fold(fbuf, S, NZ)
    setup = (exchange_copies(kbuf, ksend, krecv, peers)
             + exchange_copies(abuf.at[0], send_sem.at[0], recv_sem.at[0], peers)
             + exchange_copies(fbuf, fsend, frecv, peers))
    for copy in setup:
        copy.start()

    weights = {}
    for (a, b, c), m in INDEX.items():
        plain = w_ref[m] * (0.5 * SCALE)
        if b == 0:
            weights[(a, b, c)] = plain
        else:
            weights[(a, b, c)] = jnp.where(upright, plain, w_ref[INDEX[(a, -b, c)]] * (0.5 * SCALE))

    for copy in setup:
        copy.wait()

    def coef_block(z0, count):
        for k in range(-1, 4):
            base = PAD + 8 * k
            win = load_window(kbuf, z0 + 1, count, base)
            for z in range(count):
                mid = win[z + 1][1]
                moved = {0: mid, 1: pltpu.roll(mid, 2, 1), -1: pltpu.roll(mid, LANES - 2, 1)}
                part = {}
                for o, m in INDEX.items():
                    a, b, c = o
                    t = weights[o] * (moved[a] + win[z + 1 + c][1 + b])
                    tbuf[m, z0 + z, pl.ds(8 * (k + 1), 8), :] = t
                    part[a] = t if a not in part else part[a] + t
                diag = part[0] + pltpu.roll(part[1], LANES - 2, 1) + pltpu.roll(part[-1], 2, 1)
                inv = 1.0 / diag
                idbuf[z0 + z + 1, pl.ds(base, 8), :] = inv
                fbuf[z0 + z + 1, pl.ds(base, 8), :] = fbuf[z0 + z + 1, pl.ds(base, 8), :] * (inv * SCALE)

    rows_loop(ZE - 2, coef_block)

    def sweep(src, dst, step, omega):
        depth = S - step
        blocks = range(-1, 4) if depth else range(0, 4)
        start = S - depth

        def block(z0, count):
            z0 = z0 + start
            for k in blocks:
                base = PAD + 8 * k
                win = load_window(src, z0, count, base)
                for z in range(count):
                    part = {}
                    for (a, b, c), m in INDEX.items():
                        t = tbuf[m, z0 + z - 1, pl.ds(8 * (k + 1), 8), :] * win[z + 1 + c][1 + b]
                        part[a] = t if a not in part else part[a] + t
                    total = part[0] + pltpu.roll(part[1], LANES - 2, 1) + pltpu.roll(part[-1], 2, 1)
                    mid = win[z + 1][1]
                    at = (z0 + z, pl.ds(base, 8), slice(None))
                    new = mid + omega * (total * idbuf[at] + fbuf[at] - mid)
                    dst[at] = new
                    if k == 3:
                        dst[z0 + z, pl.ds(FOLD, 1), :] = swap_pairs(new, even)[7:8, :]

        rows_loop(NZ + 2 * depth, block)

    n_macro = n_sweeps // S

    def macro(e, p):
        for step in range(1, S + 1):
            src = abuf.at[p] if step == 1 else (bbuf if step % 2 == 0 else cbuf)
            dst = abuf.at[1 - p] if step == S else (bbuf if step % 2 == 1 else cbuf)
            sweep(src, dst, step, om_ref[e * S + step - 1])

    def body(e, carry):
        p = e % 2
        macro(e, p)
        copies = exchange_copies(abuf.at[1 - p], send_sem.at[1 - p], recv_sem.at[1 - p], peers)
        for copy in copies:
            copy.start()
        for copy in copies:
            copy.wait()
        return carry

    lax.fori_loop(0, n_macro - 1, body, 0)
    macro(n_macro - 1, (n_macro - 1) % 2)
    done = pltpu.make_async_copy(abuf.at[n_macro % 2, own[0], own[1], :], o_ref, in_sem.at[0])
    done.start()
    done.wait()


def fold_in(brick, gy):
    brick = lax.all_to_all(brick, "gx", split_axis=3, concat_axis=1, tiled=True)
    straight, mirrored = brick[:, :, :NU], brick[:, :, NU:][:, :, ::-1]
    first = jnp.where(gy == 0, straight, mirrored)
    second = jnp.where(gy == 0, mirrored, straight)
    both = jnp.stack([first, second], axis=-1)
    return both.transpose(0, 3, 2, 1, 4).reshape(brick.shape[0], NZ, NU, LANES)


def fold_out(u, gy):
    both = u.reshape(NZ, NU, LANES // 2, 2).transpose(2, 1, 0, 3)
    first, second = both[..., 0], both[..., 1]
    straight = jnp.where(gy == 0, first, second)
    mirrored = jnp.where(gy == 0, second, first)
    brick = jnp.concatenate([straight, mirrored[:, ::-1]], axis=1)
    return lax.all_to_all(brick, "gx", split_axis=0, concat_axis=2, tiled=True)


def solution(mesh):
    brick_spec = P(("batch", "gx"), "gy", "gz")

    def local_sweeps(u_brick, f_brick, kappa_brick, stencil_w, omega_sweep):
        gy = lax.axis_index("gy")
        u, f, k = fold_in(jnp.stack([u_brick, f_brick, kappa_brick]), gy)
        dma = pltpu.SemaphoreType.DMA
        plane = (ZE, ROWS, LANES)
        out = pl.pallas_call(
            functools.partial(kernel, omega_sweep.shape[0]),
            out_shape=jax.ShapeDtypeStruct((NZ, NU, LANES), jnp.float32),
            in_specs=[pl.BlockSpec(memory_space=pltpu.SMEM)] * 2 + [pl.BlockSpec(memory_space=pl.ANY)] * 3,
            out_specs=pl.BlockSpec(memory_space=pl.ANY),
            scratch_shapes=[
                pltpu.VMEM((2,) + plane, jnp.float32),
                pltpu.VMEM(plane, jnp.float32),
                pltpu.VMEM(plane, jnp.float32),
                pltpu.VMEM(plane, jnp.float32),
                pltpu.VMEM(plane, jnp.float32),
                pltpu.VMEM(plane, jnp.float32),
                pltpu.VMEM((26, ZE - 2, 40, LANES), jnp.float32),
                dma((3,)), dma((2, NCOPY)), dma((2, NCOPY)),
                dma((NCOPY,)), dma((NCOPY,)), dma((NCOPY,)), dma((NCOPY,)),
            ],
            compiler_params=pltpu.CompilerParams(
                collective_id=0, has_side_effects=True, vmem_limit_bytes=60 * 2 ** 20
            ),
        )(stencil_w, omega_sweep, u, f, k)
        return fold_out(out, gy)

    return jax.shard_map(local_sweeps, mesh=mesh, in_specs=(brick_spec, brick_spec, brick_spec, P(), P()), out_specs=brick_spec, check_vma=False)
```
